8 devices in a mesh: fsdp: 8 (over z, y, x, core).
Axes of the slice: x: 2, y: 2, z: 1, core: 2. Of those that a mesh axis runs over, the one named last changes fastest.
Arguments:
- tokens: int32 [8, 512], P('fsdp')
- embed_table: float32 [49152, 2048], P('fsdp')
- norm_gain: float32 [2048], P('fsdp')
- w_query: float32 [2048, 2048], P('fsdp')
- w_key: float32 [2048, 2048], P('fsdp')
- w_value: float32 [2048, 2048], P('fsdp')
- d_query: bfloat16 [8, 512, 2048], P('fsdp')
- d_key: bfloat16 [8, 512, 2048], P('fsdp')
- d_value: bfloat16 [8, 512, 2048], P('fsdp')
Outputs:
- output 1: bfloat16 [8, 512, 2048], P('fsdp')
- output 2: bfloat16 [8, 512, 2048], P('fsdp')
- output 3: bfloat16 [8, 512, 2048], P('fsdp')
- output 4: float32 [49152, 2048], P('fsdp')
- output 5: float32 [2048], P('fsdp')
- output 6: float32 [2048, 2048], P('fsdp')
- output 7: float32 [2048, 2048], P('fsdp')
- output 8: float32 [2048, 2048], P('fsdp')
All inputs are finite; a program needn't handle non-finite values.
Results may differ from the reference program's by a relative error of at most 0.00413466.
Values are sent between devices in bfloat16 or wider.
A program may use at most 1 GiB of HBM per device.

```python
import math
import jax
import jax.numpy as jnp
from jax import lax

VOCAB_SIZE = 49152
MODEL_DIM = 2048
NUM_HEADS = 32
KV_HEADS = 32
HEAD_DIM = 64
BATCH_SIZE = 8
SEQ_LEN = 512


def draw_tokens(tok_key):
    num_levels = int(math.ceil(math.log2(VOCAB_SIZE)))
    level_key, id_key = jax.random.split(tok_key)
    tok_shape = (BATCH_SIZE, SEQ_LEN)
    tok_level = jax.random.randint(level_key, tok_shape, 0, num_levels + 1)
    id_upper = jnp.minimum(jnp.left_shift(jnp.ones(tok_shape, jnp.int32), tok_level), VOCAB_SIZE)
    token_ids = jax.random.randint(id_key, tok_shape, 0, id_upper)
    token_ids = token_ids.at[0, 0].set(0)
    return token_ids.at[BATCH_SIZE - 1, SEQ_LEN - 1].set(VOCAB_SIZE - 1)


def setup_inputs(seed: int = 0) -> dict:
    sub_keys = jax.random.split(jax.random.key(seed), 9)
    q_width = NUM_HEADS * HEAD_DIM
    kv_width = KV_HEADS * HEAD_DIM
    w_scale = MODEL_DIM ** -0.5
    cot_scale = (BATCH_SIZE * SEQ_LEN) ** -0.5
    act_shape = (BATCH_SIZE, SEQ_LEN)
    tokens = draw_tokens(sub_keys[0])
    embed_table = jax.random.normal(sub_keys[1], (VOCAB_SIZE, MODEL_DIM), jnp.float32)
    norm_gain = 1.0 + 0.3 * jax.random.normal(sub_keys[2], (MODEL_DIM,), jnp.float32)
    w_query = w_scale * jax.random.normal(sub_keys[3], (MODEL_DIM, q_width), jnp.float32)
    w_key = w_scale * jax.random.normal(sub_keys[4], (MODEL_DIM, kv_width), jnp.float32)
    w_value = w_scale * jax.random.normal(sub_keys[5], (MODEL_DIM, kv_width), jnp.float32)
    d_query = (cot_scale * jax.random.normal(sub_keys[6], act_shape + (q_width,), jnp.float32)).astype(jnp.bfloat16)
    d_key = (cot_scale * jax.random.normal(sub_keys[7], act_shape + (kv_width,), jnp.float32)).astype(jnp.bfloat16)
    d_value = (cot_scale * jax.random.normal(sub_keys[8], act_shape + (kv_width,), jnp.float32)).astype(jnp.bfloat16)
    return dict(tokens=tokens, embed_table=embed_table, norm_gain=norm_gain, w_query=w_query, w_key=w_key, w_value=w_value, d_query=d_query, d_key=d_key, d_value=d_value)


def reference(tokens, embed_table, norm_gain, w_query, w_key, w_value, d_query, d_key, d_value):
    w_query_bf = w_query.astype(jnp.bfloat16)
    w_key_bf = w_key.astype(jnp.bfloat16)
    w_value_bf = w_value.astype(jnp.bfloat16)

    def seq_step(acc_carry, row_in):
        grad_q, grad_k, grad_v, grad_gain = acc_carry
        tok_row, dq_row, dk_row, dv_row = row_in
        x_rows = embed_table[tok_row].astype(jnp.bfloat16).astype(jnp.float32)
        inv_rms = lax.rsqrt(jnp.mean(x_rows * x_rows, axis=-1, keepdims=True) + 1e-5)
        h_rows = x_rows * inv_rms
        normed = (h_rows * norm_gain).astype(jnp.bfloat16)
        q_rows = jnp.dot(normed, w_query_bf, preferred_element_type=jnp.float32).astype(jnp.bfloat16)
        k_rows = jnp.dot(normed, w_key_bf, preferred_element_type=jnp.float32).astype(jnp.bfloat16)
        v_rows = jnp.dot(normed, w_value_bf, preferred_element_type=jnp.float32).astype(jnp.bfloat16)
        grad_q = grad_q + jnp.dot(normed.T, dq_row, preferred_element_type=jnp.float32)
        grad_k = grad_k + jnp.dot(normed.T, dk_row, preferred_element_type=jnp.float32)
        grad_v = grad_v + jnp.dot(normed.T, dv_row, preferred_element_type=jnp.float32)
        d_normed = (jnp.dot(dq_row, w_query_bf.T, preferred_element_type=jnp.float32)
                    + jnp.dot(dk_row, w_key_bf.T, preferred_element_type=jnp.float32)
                    + jnp.dot(dv_row, w_value_bf.T, preferred_element_type=jnp.float32))
        grad_gain = grad_gain + jnp.sum(d_normed * h_rows, axis=0)
        u_rows = d_normed * norm_gain
        d_x = inv_rms * (u_rows - h_rows * jnp.mean(u_rows * h_rows, axis=-1, keepdims=True))
        return (grad_q, grad_k, grad_v, grad_gain), (q_rows, k_rows, v_rows, d_x)

    acc_init = (jnp.zeros(w_query.shape, jnp.float32), jnp.zeros(w_key.shape, jnp.float32),
                jnp.zeros(w_value.shape, jnp.float32), jnp.zeros(norm_gain.shape, jnp.float32))
    grad_sums, per_row = lax.scan(seq_step, acc_init, (tokens, d_query, d_key, d_value))
    query_proj, key_proj, value_proj, d_x_all = per_row
    d_embed = jnp.zeros(embed_table.shape, jnp.float32).at[tokens].add(d_x_all)
    grad_q, grad_k, grad_v, grad_gain = grad_sums
    return (query_proj, key_proj, value_proj, d_embed, grad_gain, grad_q, grad_k, grad_v)
```

```python
import functools

import jax
import jax.numpy as jnp
from jax import lax
from jax.experimental import pallas as pl
from jax.experimental.pallas import tpu as pltpu
from jax.sharding import PartitionSpec as P

AXIS_NAME = "fsdp"
MAIN_SLOTS = 1920
NUM_CHUNKS = 4
ARRIVALS = ([[(0, c) for c in range(4)], [(1, c) for c in range(4)]]
            + [[(2, k), (4, k), (3, k), (5, k)] for k in range(4)]
            + [[(6, j), (6, j + 2), (7, j), (7, j + 2)] for j in range(2)])


def gather_and_backward_kernel(seq, dim, width3, rows_local, cot_ref, w_ref, n_ref, nst_ref, hs_ref,
                               all_ref, q_ref, dn_ref, dw_ref, dg_ref,
                               w_vm, a_vm, dn_vm, dw_vm, dg_vm,
                               recv_sem, send_sem, w_sem, load_sem, out_sem, q_sem):
    me = lax.axis_index(AXIS_NAME)
    step = seq // NUM_CHUNKS
    width = width3 // 3
    mesh_id = pl.DeviceIdType.MESH

    def remote(src, src_dev, chunk, target, sem):
        return pltpu.make_async_remote_copy(
            src_ref=src, dst_ref=all_ref.at[src_dev, pl.ds(chunk * step, step)],
            send_sem=send_sem.at[sem], recv_sem=recv_sem.at[lax.bitwise_xor(src_dev, target), chunk],
            device_id=(target,), device_id_type=mesh_id)

    def own_copy(mask, chunk):
        return remote(cot_ref.at[pl.ds(chunk * step, step)], me, chunk, me ^ mask, (mask // 2) * NUM_CHUNKS + chunk)

    def forward(mask, chunk, target_mask, sem):
        src_dev = me ^ mask
        return remote(all_ref.at[src_dev, pl.ds(chunk * step, step)], src_dev, chunk, me ^ target_mask, sem)

    def arrived(mask, chunk):
        return pltpu.make_async_remote_copy(
            src_ref=cot_ref.at[pl.ds(0, step)], dst_ref=all_ref.at[me ^ mask, pl.ds(chunk * step, step)],
            send_sem=send_sem.at[0], recv_sem=recv_sem.at[mask, chunk], device_id=(me,), device_id_type=mesh_id)

    barrier = pltpu.get_barrier_semaphore()
    for mask in (1, 2, 4):
        pl.semaphore_signal(barrier, inc=1, device_id=(me ^ mask,), device_id_type=mesh_id)
    pl.semaphore_wait(barrier, 3)

    for chunk in range(NUM_CHUNKS):
        for mask in (2, 4, 1):
            own_copy(mask, chunk).start()

    w_copies = [pltpu.make_async_copy(w_ref, w_vm, w_sem.at[0])]
    for c in w_copies:
        c.start()
    own_load = pltpu.make_async_copy(cot_ref, a_vm.at[0], load_sem.at[0])
    own_load.start()
    dw_vm[...] = jnp.zeros_like(dw_vm)
    dg_vm[...] = jnp.zeros_like(dg_vm)
    for c in w_copies:
        c.wait()

    tile_q = 512

    def q_tile(i, carry):
        cols = pl.ds(pl.multiple_of(i * tile_q, tile_q), tile_q)
        a_vm[1, :, cols] = jnp.dot(n_ref[...], w_vm[:, cols], preferred_element_type=jnp.float32).astype(jnp.bfloat16)
        return carry

    lax.fori_loop(0, width3 // tile_q, q_tile, 0)
    q_copy = [pltpu.make_async_copy(a_vm.at[1, :, pl.ds(i * width, width)], q_ref.at[i], q_sem.at[i]) for i in range(3)]
    for c in q_copy:
        c.start()
    own_load.wait()

    def load_groups(groups, buf):
        copies = [pltpu.make_async_copy(all_ref.at[me ^ mask, pl.ds(chunk * step, step)],
                                        a_vm.at[buf, pl.ds(g * step, step)], load_sem.at[g])
                  for g, (mask, chunk) in enumerate(groups)]
        for c in copies:
            c.start()
        for c in copies:
            c.wait()

    def dn_out(u):
        return pltpu.make_async_copy(dn_vm, dn_ref.at[pl.ds(u * seq, seq)], out_sem.at[0])

    def unit(u, carry):
        buf = u % 2

        @pl.when(u == 1)
        def _():
            for c in q_copy:
                c.wait()
            for chunk in range(NUM_CHUNKS):
                arrived(1, chunk).wait_recv()
            load_groups([(1, c) for c in range(NUM_CHUNKS)], buf)

        @pl.when((u >= 2) & (u < 6))
        def _():
            k = u - 2
            arrived(2, k).wait_recv()
            forward(2, k, 1, 12 + k).start()

            @pl.when(k < 2)
            def _():
                forward(2, k, 4, 24 + k).start()

            arrived(4, k).wait_recv()
            forward(4, k, 1, 16 + k).start()

            @pl.when(k >= 2)
            def _():
                forward(4, k, 2, 24 + k).start()

            arrived(3, k).wait_recv()
            arrived(5, k).wait_recv()
            load_groups([(2, k), (4, k), (3, k), (5, k)], buf)

        @pl.when(u >= 6)
        def _():
            j = u - 6
            for chunk in (j, j + 2):
                arrived(6, chunk).wait_recv()
                forward(6, chunk, 1, 20 + chunk).start()
            for chunk in (j, j + 2):
                arrived(7, chunk).wait_recv()
            load_groups([(6, j), (6, j + 2), (7, j), (7, j + 2)], buf)

        rows = pl.ds(pl.multiple_of(u * seq, seq), seq)
        tile_w = 512

        def dw_tile(i, c):
            cols = pl.ds(pl.multiple_of(i * tile_w, tile_w), tile_w)
            dw_vm[:, cols] += jnp.dot(nst_ref[:, rows], a_vm[buf, :, cols], preferred_element_type=jnp.float32)
            return c

        lax.fori_loop(0, width3 // tile_w, dw_tile, 0)

        @pl.when(u >= 1)
        def _():
            dn_out(u - 1).wait()

        def dn_tile(i, c):
            d_rows = pl.ds(pl.multiple_of(i * rows_local, rows_local), rows_local)
            acc = lax.dot_general(a_vm[buf], w_vm[d_rows, :], (((1,), (1,)), ((), ())), preferred_element_type=jnp.float32)
            dn_vm[:, d_rows] = acc

            @pl.when(i == me)
            def _():
                dg_vm[...] += jnp.sum((acc * hs_ref[rows, :]).reshape(seq // 8, 8, rows_local), axis=0)

            return c

        lax.fori_loop(0, dim // rows_local, dn_tile, 0)
        dn_out(u).start()
        return carry

    lax.fori_loop(0, 8, unit, 0)
    dw_copies = [pltpu.make_async_copy(dw_vm.at[:, pl.ds(i * width, width)], dw_ref.at[i], q_sem.at[i]) for i in range(3)]
    for c in dw_copies:
        c.start()
    dg_ref[...] = dg_vm[...]
    dn_out(7).wait()
    for c in dw_copies:
        c.wait()
    for chunk in range(NUM_CHUNKS):
        for mask in (2, 4, 1):
            own_copy(mask, chunk).wait_send()
        forward(2, chunk, 1, 12 + chunk).wait_send()
        forward(4, chunk, 1, 16 + chunk).wait_send()
        forward(6, chunk, 1, 20 + chunk).wait_send()
        forward(2 if chunk < 2 else 4, chunk, 4 if chunk < 2 else 2, 24 + chunk).wait_send()


def gather_and_backward(cot, w_full, n_home, ns_t, hs_all):
    seq, width3 = cot.shape
    dim = w_full.shape[0]
    rows_local, num_tok = ns_t.shape
    width = width3 // 3
    any_spec = pl.BlockSpec(memory_space=pl.ANY)
    vm_spec = pl.BlockSpec(memory_space=pltpu.VMEM)
    flops = 2 * num_tok * dim * width3 + 2 * num_tok * rows_local * width3 + 2 * seq * dim * width3
    return pl.pallas_call(
        functools.partial(gather_and_backward_kernel, seq, dim, width3, rows_local),
        out_shape=(jax.ShapeDtypeStruct((8, seq, width3), jnp.bfloat16),
                   jax.ShapeDtypeStruct((3, seq, width), jnp.bfloat16),
                   jax.ShapeDtypeStruct((num_tok, dim), jnp.float32),
                   jax.ShapeDtypeStruct((3, rows_local, width), jnp.float32),
                   jax.ShapeDtypeStruct((8, rows_local), jnp.float32)),
        in_specs=[any_spec, any_spec, vm_spec, vm_spec, vm_spec],
        out_specs=(any_spec, any_spec, any_spec, any_spec, vm_spec),
        scratch_shapes=[
            pltpu.VMEM((dim, width3), jnp.bfloat16),
            pltpu.VMEM((2, seq, width3), jnp.bfloat16),
            pltpu.VMEM((seq, dim), jnp.float32),
            pltpu.VMEM((rows_local, width3), jnp.float32),
            pltpu.VMEM((8, rows_local), jnp.float32),
            pltpu.SemaphoreType.DMA((8, NUM_CHUNKS)),
            pltpu.SemaphoreType.DMA((28,)),
            pltpu.SemaphoreType.DMA((1,)),
            pltpu.SemaphoreType.DMA((4,)),
            pltpu.SemaphoreType.DMA((1,)),
            pltpu.SemaphoreType.DMA((3,)),
        ],
        cost_estimate=pl.CostEstimate(flops=flops, bytes_accessed=150_000_000, transcendentals=0),
        compiler_params=pltpu.CompilerParams(collective_id=1, has_side_effects=True, vmem_limit_bytes=67_043_328),
        name="gather_and_backward",
    )(cot, w_full, n_home, ns_t, hs_all)


def solution(mesh):
    num_dev = mesh.shape[AXIS_NAME]

    def local_step(tokens, embed_shard, gain_shard, wq_shard, wk_shard, wv_shard, d_query, d_key, d_value):
        vocab_local, dim = embed_shard.shape
        rows_local, width = wq_shard.shape
        seq = tokens.shape[1]
        num_tok = num_dev * seq
        dev_index = lax.axis_index(AXIS_NAME)

        w_own = jnp.concatenate([wq_shard, wk_shard, wv_shard], axis=1).astype(jnp.bfloat16)
        w_full = lax.all_gather(w_own, AXIS_NAME, axis=0, tiled=True)
        gain_full = lax.all_gather(gain_shard, AXIS_NAME, axis=0, tiled=True)

        ids = lax.all_gather(tokens, AXIS_NAME, axis=0, tiled=True).reshape(num_tok)
        pieces = jnp.asarray([[m, c] for unit in ARRIVALS for m, c in unit], jnp.int32)
        piece_rows = (pieces[:, 0] ^ dev_index) * NUM_CHUNKS + pieces[:, 1]

        def in_arrival_order(per_token):
            return per_token.reshape(num_dev * NUM_CHUNKS, seq // NUM_CHUNKS)[piece_rows].reshape(num_tok)

        pos = jnp.arange(num_tok, dtype=jnp.int32)
        first_pos = jnp.min(jnp.where(ids[:, None] == ids[None, :], pos[None, :], num_tok), axis=1)
        is_first = first_pos == pos
        slot = jnp.sum((is_first[None, :] & (pos[None, :] < first_pos[:, None])).astype(jnp.int32), axis=1)
        num_slots = jnp.sum(is_first.astype(jnp.int32))
        slot_arr = in_arrival_order(slot)
        slot_home = lax.dynamic_slice(slot, (dev_index * seq,), (seq,))

        def rows_of(local_ids):
            owned = (local_ids >= 0) & (local_ids < vocab_local)
            rows = jnp.take(embed_shard, jnp.where(owned, local_ids, 0), axis=0).astype(jnp.bfloat16)
            return owned, jnp.where(owned[:, None], rows, jnp.zeros((), jnp.bfloat16))

        def slot_batch(base, count):
            names = base + jnp.arange(count, dtype=jnp.int32)
            uid = jnp.max(jnp.where(is_first[None, :] & (slot[None, :] == names[:, None]), ids[None, :], -1), axis=1)
            part = rows_of(uid - dev_index * vocab_local)[1]
            x_slots = lax.all_gather(lax.psum_scatter(part, AXIS_NAME, scatter_dimension=0, tiled=True),
                                     AXIS_NAME, axis=0, tiled=True)
            xf = x_slots.astype(jnp.float32)
            inv = lax.rsqrt(jnp.mean(xf * xf, axis=-1, keepdims=True) + 1e-5)
            n_slots = ((xf * inv) * gain_full).astype(jnp.bfloat16)
            hot_home = (slot_home[:, None] == names[None, :]).astype(jnp.bfloat16)
            n_home = jnp.dot(hot_home, n_slots, preferred_element_type=jnp.float32).astype(jnp.bfloat16)
            hot_all = slot_arr[:, None] == names[None, :]
            x_cols = lax.dynamic_slice(x_slots, (0, dev_index * rows_local), (count, rows_local))
            xs_all = jnp.dot(hot_all.astype(jnp.bfloat16), x_cols, preferred_element_type=jnp.float32)
            inv_all = jnp.sum(jnp.where(hot_all, inv[:, 0][None, :], 0.0), axis=1)
            return n_home, xs_all, inv_all

        main = slot_batch(0, MAIN_SLOTS)
        n_home, xs_all, inv_all = lax.cond(
            num_slots > MAIN_SLOTS,
            lambda m: jax.tree.map(jnp.add, m, slot_batch(MAIN_SLOTS, num_tok - MAIN_SLOTS)),
            lambda m: m, main)
        hs_all = xs_all * inv_all[:, None]
        ns_t = (hs_all * gain_shard[None, :]).astype(jnp.bfloat16).T

        cot = jnp.concatenate([d_query[0], d_key[0], d_value[0]], axis=1)
        _, proj, d_normed, d_w, d_gain = gather_and_backward(cot, w_full, n_home, ns_t, hs_all)

        local_ids = in_arrival_order(ids) - dev_index * vocab_local
        owned, x_own = rows_of(local_ids)
        x_own = x_own.astype(jnp.float32)
        inv_own = lax.rsqrt(jnp.mean(x_own * x_own, axis=-1, keepdims=True) + 1e-5)
        h_own = x_own * inv_own
        u_own = d_normed * gain_full
        d_x = inv_own * (u_own - h_own * jnp.mean(u_own * h_own, axis=-1, keepdims=True))
        d_embed = jnp.zeros(embed_shard.shape, jnp.float32).at[jnp.where(owned, local_ids, vocab_local)].add(d_x, mode="drop")
        return (proj[0][None], proj[1][None], proj[2][None], d_embed, jnp.sum(d_gain, axis=0), d_w[0], d_w[1], d_w[2])

    row_spec = P(AXIS_NAME, None)
    act_spec = P(AXIS_NAME, None, None)
    vec_spec = P(AXIS_NAME)
    return jax.shard_map(local_step, mesh=mesh,
                         in_specs=(row_spec, row_spec, vec_spec, row_spec, row_spec, row_spec, act_spec, act_spec, act_spec),
                         out_specs=(act_spec, act_spec, act_spec, row_spec, vec_spec, row_spec, row_spec, row_spec),
                         check_vma=False)
```
